32 devices in a mesh: inner: 2 (over y), outer: 4 (over z), head: 4 (over x, core).
Axes of the slice: x: 2, y: 2, z: 4, core: 2. Of those that a mesh axis runs over, the one named last changes fastest.
Arguments:
- queries: bfloat16 [2048, 64, 128], P(('inner', 'outer', 'head')), may hold values from -6 to 6
- key_vector_rows: bfloat16 [2048, 8, 128], P(('inner', 'outer'), 'head'), may hold values from -6 to 6
- value_vector_rows: bfloat16 [2048, 8, 128], P(('inner', 'outer'), 'head'), may hold values from -6 to 6
- grad_out: bfloat16 [2048, 64, 128], P(('inner', 'outer', 'head')), may hold values from -24 to 24
Outputs:
- query_grads: bfloat16 [2048, 64, 128], P(('inner', 'outer', 'head'))
- key_gradient_rows: bfloat16 [2048, 8, 128], P(('inner', 'outer'), 'head')
- value_gradient_rows: bfloat16 [2048, 8, 128], P(('inner', 'outer'), 'head')
The draws below stay inside these ranges and needn't reach their ends.
All inputs are finite; a program needn't handle non-finite values.
Results may differ from the reference program's by a relative error of at most 0.012.
Values may be sent and summed in bfloat16 or wider, within the bound.
No kernel may reach another device: no remote copies, remote signals or barrier semaphores. Data moves between devices by JAX's collectives and lax.ppermute only.
A program may use at most 64 MiB of HBM per device.

```python
import jax
import jax.numpy as jnp
from jax import lax

QUERY_HEADS = 64
KEY_VALUE_HEADS = 8
HEAD_WIDTH = 128
BLOCK_TOKENS = 256
SEQUENCE_TOKENS = 2048


def paired_draw(key):
    queries = jax.random.truncated_normal(jax.random.fold_in(key, 21), -6.0, 6.0, (SEQUENCE_TOKENS, QUERY_HEADS, HEAD_WIDTH), jnp.float32)
    key_vector_rows = jax.random.truncated_normal(jax.random.fold_in(key, 22), -6.0, 6.0, (SEQUENCE_TOKENS, KEY_VALUE_HEADS, HEAD_WIDTH), jnp.float32)
    return (queries, key_vector_rows)


def draw_queries(key, part):
    return paired_draw(key)[0].astype(jnp.bfloat16)


def draw_key_vector_rows(key, part):
    return paired_draw(key)[1].astype(jnp.bfloat16)


def levels(rng, dims, shards, least, largest):
    def one(position, blocks):
        heights = jax.random.uniform(jax.random.fold_in(jax.random.fold_in(rng, 6), position), (blocks,), jnp.float32, least / len(shards), largest / len(shards))
        return jnp.repeat(jnp.exp(heights), dims[position] // blocks).reshape((-1,) + (1,) * (len(dims) - position - 1))

    loudness = one(*shards[0])
    for cut in shards[1:]:
        loudness = loudness * one(*cut)
    return loudness


def noise(rng, dims, deviation, most, cuts=(), kind=jnp.bfloat16):
    entries = deviation * jax.random.normal(rng, dims, jnp.float32)
    if cuts:
        entries = entries * levels(rng, dims, cuts, -0.22, 0.18)
    return jnp.clip(entries, -most, most).astype(kind)


def setup_inputs(seed: int = 0) -> dict:
    seeds = jax.random.split(jax.random.key(seed), 5)
    queries = draw_queries(jax.random.fold_in(seeds[4], 71), 0)
    key_vector_rows = draw_key_vector_rows(jax.random.fold_in(seeds[4], 71), 0)
    value_vector_rows = noise(seeds[2], (SEQUENCE_TOKENS, KEY_VALUE_HEADS, HEAD_WIDTH), 1.0, 6.0, ((0, 8), (1, 4)))
    grad_out = noise(seeds[3], (SEQUENCE_TOKENS, QUERY_HEADS, HEAD_WIDTH), 4.0, 24.0, ((0, 32),))
    return {"queries": queries, "key_vector_rows": key_vector_rows, "value_vector_rows": value_vector_rows, "grad_out": grad_out}


def head_grads(query_part, grad_part, key_part, value_part, allowed):
    softmax_scale = query_part.shape[-1] ** -0.5
    query_wide = query_part.astype(jnp.float32)
    grad_wide = grad_part.astype(jnp.float32)
    key_wide = key_part.astype(jnp.float32)
    value_wide = value_part.astype(jnp.float32)
    scores = jnp.einsum('rgd,kd->grk', query_wide, key_wide) * softmax_scale
    scores = jnp.where(allowed[None], scores, -jnp.inf)
    highest = jnp.max(scores, axis=-1, keepdims=True)
    probs = jnp.exp(scores - highest)
    probs = probs / jnp.sum(probs, axis=-1, keepdims=True)
    probs_low = lax.optimization_barrier(probs.astype(jnp.bfloat16)).astype(jnp.float32)
    value_gradient_rows = jnp.einsum('grk,rgd->kd', probs_low, grad_wide)
    dprobs = jnp.einsum('rgd,kd->grk', grad_wide, value_wide)
    delta = jnp.sum(probs * dprobs, axis=-1, keepdims=True)
    dscores = lax.optimization_barrier((probs * (dprobs - delta)).astype(jnp.bfloat16)).astype(jnp.float32)
    query_grads = jnp.einsum('grk,kd->rgd', dscores, key_wide) * softmax_scale
    key_gradient_rows = jnp.einsum('grk,rgd->kd', dscores, query_wide) * softmax_scale
    return query_grads, key_gradient_rows, value_gradient_rows


def block_grads(query_rows, grad_rows, key_window, value_window, allowed):
    row_count, head_count, width = query_rows.shape
    group_count = key_window.shape[1]
    heads_per_group = head_count // group_count
    query_split = query_rows.reshape(row_count, group_count, heads_per_group, width).transpose(1, 0, 2, 3)
    grad_split = grad_rows.reshape(row_count, group_count, heads_per_group, width).transpose(1, 0, 2, 3)
    key_split = key_window.transpose(1, 0, 2)
    value_split = value_window.transpose(1, 0, 2)
    query_grads, key_gradient_rows, value_gradient_rows = lax.map(lambda packed: head_grads(packed[0], packed[1], packed[2], packed[3], allowed), (query_split, grad_split, key_split, value_split))
    query_grads = query_grads.transpose(1, 0, 2, 3).reshape(row_count, head_count, width)
    return query_grads, key_gradient_rows.transpose(1, 0, 2), value_gradient_rows.transpose(1, 0, 2)


def reference(queries, key_vector_rows, value_vector_rows, grad_out):
    blocks = SEQUENCE_TOKENS // BLOCK_TOKENS
    query_blocks = queries.reshape(blocks, BLOCK_TOKENS, QUERY_HEADS, HEAD_WIDTH)
    grad_blocks = grad_out.reshape(blocks, BLOCK_TOKENS, QUERY_HEADS, HEAD_WIDTH)
    padding_rows = jnp.zeros((2 * BLOCK_TOKENS, KEY_VALUE_HEADS, HEAD_WIDTH), jnp.bfloat16)
    key_padded = jnp.concatenate([padding_rows, key_vector_rows], axis=0)
    value_padded = jnp.concatenate([padding_rows, value_vector_rows], axis=0)

    def step(carry, index):
        first_k, first_v, second_k, second_v = carry
        start = (index * BLOCK_TOKENS).astype(jnp.int32)
        key_window = lax.dynamic_slice_in_dim(key_padded, start, 3 * BLOCK_TOKENS, 0)
        value_window = lax.dynamic_slice_in_dim(value_padded, start, 3 * BLOCK_TOKENS, 0)
        query_positions = index * BLOCK_TOKENS + jnp.arange(BLOCK_TOKENS, dtype=jnp.int32)
        key_positions = (index - 2) * BLOCK_TOKENS + jnp.arange(3 * BLOCK_TOKENS, dtype=jnp.int32)
        allowed = (key_positions[None, :] <= query_positions[:, None]) & (key_positions[None, :] >= 0)
        query_block = lax.dynamic_index_in_dim(query_blocks, index, 0, keepdims=False)
        grad_block = lax.dynamic_index_in_dim(grad_blocks, index, 0, keepdims=False)
        query_grads, key_gradient_rows, value_gradient_rows = block_grads(query_block, grad_block, key_window, value_window, allowed)
        key_slot_rows = key_gradient_rows.reshape(3, BLOCK_TOKENS, KEY_VALUE_HEADS, HEAD_WIDTH)
        value_slot_rows = value_gradient_rows.reshape(3, BLOCK_TOKENS, KEY_VALUE_HEADS, HEAD_WIDTH)
        finished = (first_k + key_slot_rows[0], first_v + value_slot_rows[0])
        carry_next = (second_k + key_slot_rows[1], second_v + value_slot_rows[1], key_slot_rows[2], value_slot_rows[2])
        return carry_next, (query_grads.astype(jnp.bfloat16), finished[0], finished[1])

    zero_filled = jnp.zeros((BLOCK_TOKENS, KEY_VALUE_HEADS, HEAD_WIDTH), jnp.float32)
    final_result, output_list = lax.scan(step, (zero_filled, zero_filled, zero_filled, zero_filled), jnp.arange(blocks, dtype=jnp.int32))
    query_grads = output_list[0].reshape(SEQUENCE_TOKENS, QUERY_HEADS, HEAD_WIDTH)
    key_gradient_rows = jnp.concatenate([output_list[1][2:].reshape(-1, KEY_VALUE_HEADS, HEAD_WIDTH), final_result[0], final_result[2]], axis=0)
    value_gradient_rows = jnp.concatenate([output_list[2][2:].reshape(-1, KEY_VALUE_HEADS, HEAD_WIDTH), final_result[1], final_result[3]], axis=0)
    return query_grads, key_gradient_rows.astype(jnp.bfloat16), value_gradient_rows.astype(jnp.bfloat16)
```

```python
import functools
import math

import jax
import jax.numpy as jnp
from jax import lax
from jax.experimental import pallas as pl
from jax.experimental.pallas import tpu as pltpu
from jax.sharding import PartitionSpec as P

NT = (((1,), (1,)), ((), ()))
SEQ = ("inner", "outer")
NEVER = 1e30


def shifted(value, by):
    peers = lax.axis_size(SEQ)
    pairs = [(i, i + by) for i in range(peers) if 0 <= i + by < peers]
    return lax.ppermute(value, SEQ, pairs)


def grads_kernel(
    group, bias_ref, q_ref, do_ref, far_ref, near_ref, own_ref,
    dq_ref, dfar_ref, dnear_ref, down_ref, acc, kt,
):
    step = pl.program_id(1)
    rows, width = q_ref.shape
    tok_rows = own_ref.shape[1]
    scale = width ** (-0.5)
    to_exp2 = scale * math.log2(math.e)
    windows = (far_ref, near_ref, own_ref)

    @pl.when(step == 0)
    def _():
        acc[...] = jnp.zeros_like(acc)
        for j, window in enumerate(windows):
            kt[j] = window[0].T

    q = q_ref[...]
    do = do_ref[...]
    bias = (bias_ref[0], bias_ref[1], 0.0)
    scores, tops = [], []
    for j, window in enumerate(windows):
        s = lax.dot_general(window[0], q, NT, preferred_element_type=jnp.float32)
        if j == 2:
            token = (lax.broadcasted_iota(jnp.int32, s.shape, 1) + step * rows) // group
            key = lax.broadcasted_iota(jnp.int32, s.shape, 0)
            s = jnp.where(key <= token, s, -jnp.inf)
        scores.append(s)
        tops.append(jnp.max(s, axis=0, keepdims=True) - bias[j])
    top = jnp.maximum(jnp.maximum(tops[0], tops[1]), tops[2]) * to_exp2
    weights, dprobs, total, dtotal = [], [], 0.0, 0.0
    for j, window in enumerate(windows):
        e = jnp.exp2(scores[j] * to_exp2 - (top + bias[j]))
        dp = lax.dot_general(window[1], do, NT, preferred_element_type=jnp.float32)
        total = total + jnp.sum(e, axis=0, keepdims=True)
        dtotal = dtotal + jnp.sum(e * dp, axis=0, keepdims=True)
        weights.append(e)
        dprobs.append(dp)
    inverse = 1.0 / total
    delta = dtotal * inverse
    dqt = 0.0
    for j in range(3):
        p = weights[j] * inverse
        ds = (p * (dprobs[j] - delta)).astype(jnp.bfloat16)
        acc[j, 1] += jnp.dot(p.astype(jnp.bfloat16), do, preferred_element_type=jnp.float32)
        acc[j, 0] += jnp.dot(ds, q, preferred_element_type=jnp.float32)
        dqt = dqt + jnp.dot(kt[j], ds, preferred_element_type=jnp.float32)
    dq_ref[...] = (dqt * scale).T.astype(dq_ref.dtype)

    @pl.when(step == pl.num_programs(1) - 1)
    def _():
        for j, out in enumerate((dfar_ref, dnear_ref, down_ref)):
            out[0] = (acc[j, 0] * scale).astype(out.dtype)
            out[1] = acc[j, 1].astype(out.dtype)


def group_grads(bias, pairs, far, near, own, group):
    sources, kv_heads, _, rows, width = pairs.shape
    tok_rows = own.shape[2]
    window = pl.BlockSpec((None, 2, tok_rows, width), lambda h, i: (h, 0, 0, 0))

    def half(which):
        return pl.BlockSpec((None, None, None, rows, width), lambda h, i: (i, h, which, 0, 0))

    shape = (kv_heads, 2, tok_rows, width)
    steps = kv_heads * sources * rows * 3 * tok_rows
    return pl.pallas_call(
        functools.partial(grads_kernel, group),
        grid=(kv_heads, sources),
        in_specs=[pl.BlockSpec(memory_space=pltpu.SMEM), half(0), half(1), window, window, window],
        out_specs=[
            pl.BlockSpec((None, None, rows, width), lambda h, i: (i, h, 0, 0)),
            window, window, window,
        ],
        out_shape=[
            jax.ShapeDtypeStruct((sources, kv_heads, rows, width), jnp.bfloat16),
            jax.ShapeDtypeStruct(shape, jnp.bfloat16),
            jax.ShapeDtypeStruct(shape, jnp.bfloat16),
            jax.ShapeDtypeStruct(shape, jnp.float32),
        ],
        scratch_shapes=[
            pltpu.VMEM((3, 2, tok_rows, width), jnp.float32),
            pltpu.VMEM((3, width, tok_rows), jnp.bfloat16),
        ],
        compiler_params=pltpu.CompilerParams(dimension_semantics=("arbitrary", "arbitrary")),
        cost_estimate=pl.CostEstimate(
            flops=10 * steps * width, bytes_accessed=8 * sources * rows * width, transcendentals=steps
        ),
        name="grads",
    )(bias, pairs, pairs, far, near, own)


def shards(queries, key_vector_rows, value_vector_rows, grad_out):
    part_rows, heads, width = queries.shape
    tok_rows, kv_heads, _ = key_vector_rows.shape
    peers = lax.axis_size("head")
    group = heads // (peers * kv_heads)
    block_index = lax.axis_index(SEQ)
    bias = jnp.where(block_index < jnp.array([2, 1]), NEVER, 0.0).astype(jnp.float32)

    def by_peer(value):
        return value.reshape(part_rows, peers, kv_heads, group, width).transpose(1, 2, 0, 3, 4)

    pairs = jnp.stack([by_peer(queries), by_peer(grad_out)], axis=2)
    pairs = pairs.reshape(peers, kv_heads, 2, part_rows * group, width)
    pairs = lax.all_to_all(pairs, "head", split_axis=0, concat_axis=0, tiled=True)
    own = jnp.stack([key_vector_rows.transpose(1, 0, 2), value_vector_rows.transpose(1, 0, 2)], axis=1)
    far = shifted(own, 2)
    near = shifted(own, 1)
    dq, dfar, dnear, down = group_grads(bias, pairs, far, near, own, group)
    dq = lax.all_to_all(dq, "head", split_axis=0, concat_axis=0, tiled=True)
    dq = dq.reshape(peers, kv_heads, part_rows, group, width).transpose(2, 0, 1, 3, 4)
    total = down + shifted(dnear, -1).astype(jnp.float32) + shifted(dfar, -2).astype(jnp.float32)
    total = total.astype(jnp.bfloat16).transpose(1, 2, 0, 3)
    return dq.reshape(part_rows, heads, width), total[0], total[1]


def solution(mesh):
    return jax.shard_map(
        shards,
        mesh=mesh,
        in_specs=(
            P(("inner", "outer", "head"), None, None),
            P(("inner", "outer"), "head", None),
            P(("inner", "outer"), "head", None),
            P(("inner", "outer", "head"), None, None),
        ),
        out_specs=(
            P(("inner", "outer", "head"), None, None),
            P(("inner", "outer"), "head", None),
            P(("inner", "outer"), "head", None),
        ),
        check_vma=False,
    )
```

```python
import functools
import math

import jax
import jax.numpy as jnp
from jax import lax
from jax.experimental import pallas as pl
from jax.experimental.pallas import tpu as pltpu
from jax.sharding import PartitionSpec as P


NT = (((1,), (1,)), ((), ()))
SEQ = ("inner", "outer")
NEVER = 1e30
VMEM = pl.BlockSpec(memory_space=pltpu.VMEM)
HBM = pl.BlockSpec(memory_space=pltpu.HBM)


def shifted(value, by):
    peers = lax.axis_size(SEQ)
    pairs = [(i, i + by) for i in range(peers) if 0 <= i + by < peers]
    return lax.ppermute(value, SEQ, pairs)


def swapped(value, distance):
    peers = lax.axis_size("head")
    return lax.ppermute(value, "head", [(i, i ^ distance) for i in range(peers)])


def pack_kernel(parts, q_ref, do_ref, *refs):
    outs, sem = refs[:-1], refs[-1]
    me = lax.axis_index("head")
    kv_heads = q_ref.shape[1] // lax.axis_size("head")
    copies = []
    for out, part in zip(outs, parts):
        for n, (kv, distance) in enumerate(part):
            place = (me ^ distance) * kv_heads + kv
            for which, source in enumerate((q_ref, do_ref)):
                copies.append(
                    pltpu.make_async_copy(source.at[:, place], out.at[n, which], sem.at[len(copies)])
                )
    for copy in copies:
        copy.start()
    for copy in copies:
        copy.wait()


def pack(queries, grad_out, parts):
    part_rows, _, group, width = queries.shape
    return pl.pallas_call(
        functools.partial(pack_kernel, parts),
        in_specs=[HBM, HBM],
        out_specs=[VMEM] * len(parts),
        out_shape=[
            jax.ShapeDtypeStruct((len(part), 2, part_rows, group, width), queries.dtype)
            for part in parts
        ],
        scratch_shapes=[pltpu.SemaphoreType.DMA((2 * sum(len(part) for part in parts),))],
        compiler_params=pltpu.CompilerParams(vmem_limit_bytes=16 * 2**20),
        name="pack",
    )(queries, grad_out)


def unpack_kernel(parts, *refs):
    values, out_ref, sem = refs[:-2], refs[-2], refs[-1]
    me = lax.axis_index("head")
    kv_heads = out_ref.shape[1] // lax.axis_size("head")
    copies = []
    for value, part in zip(values, parts):
        for n, (kv, distance) in enumerate(part):
            place = (me ^ distance) * kv_heads + kv
            copies.append(
                pltpu.make_async_copy(value.at[n], out_ref.at[:, place], sem.at[len(copies)])
            )
    for copy in copies:
        copy.start()
    for copy in copies:
        copy.wait()


def unpack(values, parts, places):
    _, part_rows, group, width = values[0].shape
    return pl.pallas_call(
        functools.partial(unpack_kernel, parts),
        in_specs=[VMEM] * len(values),
        out_specs=HBM,
        out_shape=jax.ShapeDtypeStruct((part_rows, places, group, width), values[0].dtype),
        scratch_shapes=[pltpu.SemaphoreType.DMA((sum(len(part) for part in parts),))],
        compiler_params=pltpu.CompilerParams(vmem_limit_bytes=16 * 2**20),
        name="unpack",
    )(*values)


def grads_kernel(where, *refs):
    peers = len(where)
    pair_refs, (far_ref, near_ref, own_ref) = refs[:peers], refs[peers : peers + 3]
    dq_refs, (dfar_ref, dnear_ref, down_ref) = (
        refs[peers + 3 : 2 * peers + 3],
        refs[2 * peers + 3 : 2 * peers + 6],
    )
    pairs, dqs, acc, kt = refs[2 * peers + 6 :]
    windows = (far_ref, near_ref, own_ref)
    _, part_rows, group, width = pair_refs[0].shape[1:]
    rows = part_rows * group
    scale = width ** (-0.5)
    to_exp2 = scale * math.log2(math.e)
    me = lax.axis_index("head")
    block = lax.axis_index(SEQ)
    bias = (
        jnp.where(block < 2, NEVER, 0.0).astype(jnp.float32),
        jnp.where(block < 1, NEVER, 0.0).astype(jnp.float32),
        0.0,
    )
    for d in range(peers):
        pairs[d] = pair_refs[d][where[d]].reshape(2, rows, width)
    for j, window in enumerate(windows):
        kt[j] = window[0].T
    acc[...] = jnp.zeros_like(acc)

    def step(d, carry):
        q = pairs[d, 0]
        do = pairs[d, 1]
        first = (me ^ d) * rows
        scores, tops = [], []
        for j, window in enumerate(windows):
            s = lax.dot_general(window[0], q, NT, preferred_element_type=jnp.float32)
            if j == 2:
                token = (lax.broadcasted_iota(jnp.int32, s.shape, 1) + first) // group
                key = lax.broadcasted_iota(jnp.int32, s.shape, 0)
                s = jnp.where(key <= token, s, -jnp.inf)
            scores.append(s)
            tops.append(jnp.max(s, axis=0, keepdims=True) - bias[j])
        top = jnp.maximum(jnp.maximum(tops[0], tops[1]), tops[2]) * to_exp2
        weights, dprobs, total, dtotal = [], [], 0.0, 0.0
        for j, window in enumerate(windows):
            e = jnp.exp2(scores[j] * to_exp2 - (top + bias[j]))
            dp = lax.dot_general(window[1], do, NT, preferred_element_type=jnp.float32)
            total = total + jnp.sum(e, axis=0, keepdims=True)
            dtotal = dtotal + jnp.sum(e * dp, axis=0, keepdims=True)
            weights.append(e)
            dprobs.append(dp)
        inverse = 1.0 / total
        delta = dtotal * inverse
        dqt = 0.0
        for j in range(3):
            p = weights[j] * inverse
            ds = (p * (dprobs[j] - delta)).astype(jnp.bfloat16)
            acc[j, 1] += jnp.dot(p.astype(jnp.bfloat16), do, preferred_element_type=jnp.float32)
            acc[j, 0] += jnp.dot(ds, q, preferred_element_type=jnp.float32)
            dqt = dqt + jnp.dot(kt[j], ds, preferred_element_type=jnp.float32)
        dqs[d] = (dqt * scale).T.astype(dqs.dtype)
        return carry

    lax.fori_loop(0, peers, step, 0)
    for d in range(peers):
        dq_refs[d][0] = dqs[d].reshape(part_rows, group, width)
    for j, out in enumerate((dfar_ref, dnear_ref, down_ref)):
        out[0] = (acc[j, 0] * scale).astype(out.dtype)
        out[1] = acc[j, 1].astype(out.dtype)


def group_grads(pairs, where, far, near, own):
    peers = len(pairs)
    _, _, part_rows, group, width = pairs[0].shape
    tok_rows = own.shape[1]
    rows = part_rows * group
    window = (2, tok_rows, width)
    cells = peers * rows * 3 * tok_rows
    outs = pl.pallas_call(
        functools.partial(grads_kernel, where),
        in_specs=[VMEM] * (peers + 3),
        out_specs=[VMEM] * (peers + 3),
        out_shape=[jax.ShapeDtypeStruct((1, part_rows, group, width), jnp.bfloat16)] * peers
        + [
            jax.ShapeDtypeStruct(window, jnp.bfloat16),
            jax.ShapeDtypeStruct(window, jnp.bfloat16),
            jax.ShapeDtypeStruct(window, jnp.float32),
        ],
        scratch_shapes=[
            pltpu.VMEM((peers, 2, rows, width), jnp.bfloat16),
            pltpu.VMEM((peers, rows, width), jnp.bfloat16),
            pltpu.VMEM((3, 2, tok_rows, width), jnp.float32),
            pltpu.VMEM((3, width, tok_rows), jnp.bfloat16),
        ],
        compiler_params=pltpu.CompilerParams(vmem_limit_bytes=32 * 2**20),
        cost_estimate=pl.CostEstimate(
            flops=10 * cells * width, bytes_accessed=6 * peers * rows * width, transcendentals=cells
        ),
        name="grads",
    )(*pairs, far, near, own)
    return outs[:peers], outs[peers:]


def shards(queries, key_vector_rows, value_vector_rows, grad_out):
    part_rows, heads, width = queries.shape
    kv_heads = key_vector_rows.shape[1]
    peers = lax.axis_size("head")
    group = heads // (peers * kv_heads)
    places = peers * kv_heads
    queries = queries.reshape(part_rows, places, group, width)
    grad_out = grad_out.reshape(part_rows, places, group, width)
    far_cores = list(range(2, peers))
    all_kv = list(range(kv_heads))

    first = pack(queries, grad_out, [[(0, d)] for d in far_cores])
    rest = pack(
        queries,
        grad_out,
        [[(kv, 0) for kv in all_kv], [(kv, 1) for kv in all_kv]]
        + [[(kv, d)] for kv in all_kv[1:] for d in far_cores],
    )
    sent = [first] + [rest[2 + n * len(far_cores) :][: len(far_cores)] for n in range(kv_heads - 1)]
    crossed, windows = [], []
    for kv in all_kv:
        values = []
        for value, d in zip(sent[kv], far_cores):
            values.append(swapped(value, d))
        crossed.append(values)
        own = jnp.stack([key_vector_rows[:, kv], value_vector_rows[:, kv]], axis=0)
        far = shifted(own, 2)
        near = shifted(own, 1)
        windows.append((far, near, own))
    here = rest[0]
    partner = swapped(rest[1], 1)
    dq_here, dq_partner, dq_crossed, dkeys, dvalues = [], [], [], [], []
    for kv in all_kv:
        dq, (dfar, dnear, down) = group_grads(
            [here, partner] + crossed[kv], [kv, kv] + [0] * len(far_cores), *windows[kv]
        )
        dfar = shifted(dfar, -2)
        dnear = shifted(dnear, -1)
        dq_here.append(dq[0])
        dq_partner.append(dq[1])
        values = []
        for value, d in zip(dq[2:], far_cores):
            values.append(swapped(value, d))
        dq_crossed.append(values)
        total = down + dfar.astype(jnp.float32) + dnear.astype(jnp.float32)
        total = total.astype(jnp.bfloat16)
        dkeys.append(total[0])
        dvalues.append(total[1])
    dq_partner = swapped(jnp.concatenate(dq_partner, axis=0), 1)
    values = dq_here + [dq_partner] + sum(dq_crossed, [])
    parts = [[(kv, 0)] for kv in all_kv] + [[(kv, 1) for kv in all_kv]]
    parts += [[(kv, d)] for kv in all_kv for d in far_cores]
    query_grads = unpack(values, parts, places)
    return (
        query_grads.reshape(part_rows, heads, width),
        jnp.stack(dkeys, axis=1),
        jnp.stack(dvalues, axis=1),
    )


def solution(mesh):
    return jax.shard_map(
        shards,
        mesh=mesh,
        in_specs=(
            P(("inner", "outer", "head"), None, None),
            P(("inner", "outer"), "head", None),
            P(("inner", "outer"), "head", None),
            P(("inner", "outer", "head"), None, None),
        ),
        out_specs=(
            P(("inner", "outer", "head"), None, None),
            P(("inner", "outer"), "head", None),
            P(("inner", "outer"), "head", None),
        ),
        check_vma=False,
    )
```

```python
import functools
import math

import jax
import jax.numpy as jnp
from jax import lax
from jax.experimental import pallas as pl
from jax.experimental.pallas import tpu as pltpu
from jax.sharding import PartitionSpec as P


NT = (((1,), (1,)), ((), ()))
SEQ = ("inner", "outer")
NEVER = 1e30
VMEM = pl.BlockSpec(memory_space=pltpu.VMEM)
HBM = pl.BlockSpec(memory_space=pltpu.HBM)


def shifted(value, by):
    peers = lax.axis_size(SEQ)
    pairs = [(i, (i + by) % peers) for i in range(peers)]
    return lax.ppermute(value, SEQ, pairs)


def swapped(value, distance):
    peers = lax.axis_size("head")
    return lax.ppermute(value, "head", [(i, i ^ distance) for i in range(peers)])


def in_hbm(value):
    return pltpu.with_memory_space_constraint(value, pltpu.HBM)


def pack_copies(parts, sources, outs, sem, kv_heads):
    me = lax.axis_index("head")
    copies = []
    for out, part in zip(outs, parts):
        for n, (kv, distance) in enumerate(part):
            place = (me ^ distance) * kv_heads + kv
            for which, source in enumerate(sources):
                copies.append(
                    pltpu.make_async_copy(source.at[:, place], out.at[n, which], sem.at[len(copies)])
                )
    return copies


def pack_kernel(parts, kv_heads, q_ref, do_ref, *refs):
    copies = pack_copies(parts, (q_ref, do_ref), refs[:-1], refs[-1], kv_heads)
    for copy in copies:
        copy.start()
    for copy in copies:
        copy.wait()


def first_kernel(parts, kv_heads, key_ref, value_ref, q_ref, do_ref, *refs):
    own_refs, outs = refs[:kv_heads], refs[kv_heads:-4]
    narrow, wide, own_sem, sem = refs[-4:]
    loads = [
        pltpu.make_async_copy(source, narrow.at[which], own_sem.at[which])
        for which, source in enumerate((key_ref, value_ref))
    ]
    copies = pack_copies(parts, (q_ref, do_ref), outs, sem, kv_heads)
    for copy in loads + copies:
        copy.start()
    tok_rows = own_refs[0].shape[1]
    for which, load in enumerate(loads):
        load.wait()
        wide[which] = narrow[which].astype(jnp.float32)
        for kv in range(kv_heads):
            rows = wide[which, pl.ds(kv, tok_rows, stride=kv_heads), :]
            own_refs[kv][which] = rows.astype(own_refs[kv].dtype)
    for copy in copies:
        copy.wait()


def pack(queries, grad_out, parts, kv_heads):
    part_rows, _, group, width = queries.shape
    return pl.pallas_call(
        functools.partial(pack_kernel, parts, kv_heads),
        in_specs=[HBM, HBM],
        out_specs=[VMEM] * len(parts),
        out_shape=[
            pltpu.VMEM((len(part), 2, part_rows, group, width), queries.dtype) for part in parts
        ],
        scratch_shapes=[pltpu.SemaphoreType.DMA((2 * sum(len(part) for part in parts),))],
        compiler_params=pltpu.CompilerParams(vmem_limit_bytes=16 * 2**20),
        name="pack",
    )(in_hbm(queries), in_hbm(grad_out))


def pack_first(keys, values, queries, grad_out, parts):
    tok_rows, kv_heads, width = keys.shape
    part_rows, _, group, _ = queries.shape
    outs = pl.pallas_call(
        functools.partial(first_kernel, parts, kv_heads),
        in_specs=[HBM] * 4,
        out_specs=[VMEM] * (len(parts) + kv_heads),
        out_shape=[pltpu.VMEM((2, tok_rows, width), keys.dtype)] * kv_heads
        + [pltpu.VMEM((len(part), 2, part_rows, group, width), queries.dtype) for part in parts],
        scratch_shapes=[
            pltpu.VMEM((2, tok_rows * kv_heads, width), keys.dtype),
            pltpu.VMEM((2, tok_rows * kv_heads, width), jnp.float32),
            pltpu.SemaphoreType.DMA((2,)),
            pltpu.SemaphoreType.DMA((2 * sum(len(part) for part in parts),)),
        ],
        compiler_params=pltpu.CompilerParams(vmem_limit_bytes=16 * 2**20),
        name="first",
    )(
        in_hbm(keys.reshape(tok_rows * kv_heads, width)),
        in_hbm(values.reshape(tok_rows * kv_heads, width)),
        in_hbm(queries),
        in_hbm(grad_out),
    )
    return outs[:kv_heads], outs[kv_heads:]


def finish_kernel(parts, heads, *refs):
    values, totals = refs[: len(parts)], refs[len(parts) : len(parts) + 3 * heads]
    dq_ref, dk_ref, dv_ref, wide, narrow, sem = refs[len(parts) + 3 * heads :]
    me = lax.axis_index("head")
    copies = []
    for value, part in zip(values, parts):
        for n, (kv, distance) in enumerate(part):
            place = (me ^ distance) * heads + kv
            copies.append(
                pltpu.make_async_copy(value.at[n], dq_ref.at[:, place], sem.at[len(copies)])
            )
    for copy in copies:
        copy.start()
    tok_rows = totals[0].shape[1]
    for which, out in enumerate((dk_ref, dv_ref)):
        for kv in range(heads):
            own, far, near = totals[3 * kv : 3 * kv + 3]
            total = own[which] + far[which].astype(jnp.float32) + near[which].astype(jnp.float32)
            wide[which, pl.ds(kv, tok_rows, stride=heads), :] = total
        narrow[which] = wide[which].astype(narrow.dtype)
        copies.append(pltpu.make_async_copy(narrow.at[which], out, sem.at[len(copies)]))
        copies[-1].start()
    for copy in copies:
        copy.wait()


def finish(values, parts, totals):
    _, part_rows, group, width = values[0].shape
    heads = len(totals)
    tok_rows = totals[0][0].shape[1]
    places = sum(len(part) for part in parts)
    dq, dk, dv = pl.pallas_call(
        functools.partial(finish_kernel, parts, heads),
        in_specs=[VMEM] * (len(values) + 3 * heads),
        out_specs=[HBM] * 3,
        out_shape=[
            jax.ShapeDtypeStruct((part_rows, places, group, width), jnp.bfloat16),
            jax.ShapeDtypeStruct((tok_rows * heads, width), jnp.bfloat16),
            jax.ShapeDtypeStruct((tok_rows * heads, width), jnp.bfloat16),
        ],
        scratch_shapes=[
            pltpu.VMEM((2, tok_rows * heads, width), jnp.float32),
            pltpu.VMEM((2, tok_rows * heads, width), jnp.bfloat16),
            pltpu.SemaphoreType.DMA((places + 2,)),
        ],
        compiler_params=pltpu.CompilerParams(vmem_limit_bytes=16 * 2**20),
        name="finish",
    )(*values, *(term for total in totals for term in total))
    return (
        dq.reshape(part_rows, places * group, width),
        dk.reshape(tok_rows, heads, width),
        dv.reshape(tok_rows, heads, width),
    )


def grads_kernel(where, *refs):
    peers = len(where)
    pair_refs, (far_ref, near_ref, own_ref) = refs[:peers], refs[peers : peers + 3]
    dq_refs, (dfar_ref, dnear_ref, down_ref) = (
        refs[peers + 3 : 2 * peers + 3],
        refs[2 * peers + 3 : 2 * peers + 6],
    )
    pairs, dqs, acc, kt = refs[2 * peers + 6 :]
    windows = (far_ref, near_ref, own_ref)
    _, part_rows, group, width = pair_refs[0].shape[1:]
    rows = part_rows * group
    scale = width ** (-0.5)
    to_exp2 = scale * math.log2(math.e)
    me = lax.axis_index("head")
    block = lax.axis_index(SEQ)
    bias = (
        jnp.where(block < 2, NEVER, 0.0).astype(jnp.float32),
        jnp.where(block < 1, NEVER, 0.0).astype(jnp.float32),
        0.0,
    )
    for d in range(peers):
        pairs[d] = pair_refs[d][where[d]].reshape(2, rows, width)
    for j, window in enumerate(windows):
        kt[j] = window[0].T
    acc[...] = jnp.zeros_like(acc)

    def step(d, carry):
        q = pairs[d, 0]
        do = pairs[d, 1]
        first = (me ^ d) * rows
        scores, tops = [], []
        for j, window in enumerate(windows):
            s = lax.dot_general(window[0], q, NT, preferred_element_type=jnp.float32)
            if j == 2:
                token = (lax.broadcasted_iota(jnp.int32, s.shape, 1) + first) // group
                key = lax.broadcasted_iota(jnp.int32, s.shape, 0)
                s = jnp.where(key <= token, s, -jnp.inf)
            scores.append(s)
            tops.append(jnp.max(s, axis=0, keepdims=True) - bias[j])
        top = jnp.maximum(jnp.maximum(tops[0], tops[1]), tops[2]) * to_exp2
        weights, dprobs, total, dtotal = [], [], 0.0, 0.0
        for j, window in enumerate(windows):
            e = jnp.exp2(scores[j] * to_exp2 - (top + bias[j]))
            dp = lax.dot_general(window[1], do, NT, preferred_element_type=jnp.float32)
            total = total + jnp.sum(e, axis=0, keepdims=True)
            dtotal = dtotal + jnp.sum(e * dp, axis=0, keepdims=True)
            weights.append(e)
            dprobs.append(dp)
        inverse = 1.0 / total
        delta = dtotal * inverse
        dqt = 0.0
        for j in range(3):
            p = weights[j] * inverse
            ds = (p * (dprobs[j] - delta)).astype(jnp.bfloat16)
            acc[j, 1] += jnp.dot(p.astype(jnp.bfloat16), do, preferred_element_type=jnp.float32)
            acc[j, 0] += jnp.dot(ds, q, preferred_element_type=jnp.float32)
            dqt = dqt + jnp.dot(kt[j], ds, preferred_element_type=jnp.float32)
        dqs[d] = (dqt * scale).T.astype(dqs.dtype)
        return carry

    lax.fori_loop(0, peers, step, 0)
    for d in range(peers):
        dq_refs[d][0] = dqs[d].reshape(part_rows, group, width)
    for j, out in enumerate((dfar_ref, dnear_ref, down_ref)):
        out[0] = (acc[j, 0] * scale).astype(out.dtype)
        out[1] = acc[j, 1].astype(out.dtype)


def group_grads(pairs, where, far, near, own):
    peers = len(pairs)
    _, _, part_rows, group, width = pairs[0].shape
    tok_rows = own.shape[1]
    rows = part_rows * group
    window = (2, tok_rows, width)
    cells = peers * rows * 3 * tok_rows
    outs = pl.pallas_call(
        functools.partial(grads_kernel, where),
        in_specs=[VMEM] * (peers + 3),
        out_specs=[VMEM] * (peers + 3),
        out_shape=[jax.ShapeDtypeStruct((1, part_rows, group, width), jnp.bfloat16)] * peers
        + [
            jax.ShapeDtypeStruct(window, jnp.bfloat16),
            jax.ShapeDtypeStruct(window, jnp.bfloat16),
            jax.ShapeDtypeStruct(window, jnp.float32),
        ],
        scratch_shapes=[
            pltpu.VMEM((peers, 2, rows, width), jnp.bfloat16),
            pltpu.VMEM((peers, rows, width), jnp.bfloat16),
            pltpu.VMEM((3, 2, tok_rows, width), jnp.float32),
            pltpu.VMEM((3, width, tok_rows), jnp.bfloat16),
        ],
        compiler_params=pltpu.CompilerParams(vmem_limit_bytes=32 * 2**20),
        cost_estimate=pl.CostEstimate(
            flops=10 * cells * width, bytes_accessed=6 * peers * rows * width, transcendentals=cells
        ),
        name="grads",
    )(*pairs, far, near, own)
    return outs[:peers], outs[peers:]


def shards(queries, key_vector_rows, value_vector_rows, grad_out):
    part_rows, heads, width = queries.shape
    kv_heads = key_vector_rows.shape[1]
    peers = lax.axis_size("head")
    group = heads // (peers * kv_heads)
    places = peers * kv_heads
    queries = queries.reshape(part_rows, places, group, width)
    grad_out = grad_out.reshape(part_rows, places, group, width)
    far_cores = list(range(2, peers))
    all_kv = list(range(kv_heads))

    own, first = pack_first(
        key_vector_rows, value_vector_rows, queries, grad_out, [[(0, d)] for d in far_cores]
    )
    rest = pack(
        queries,
        grad_out,
        [[(kv, 0) for kv in all_kv], [(kv, 1) for kv in all_kv]]
        + [[(kv, d)] for kv in all_kv[1:] for d in far_cores],
        kv_heads,
    )
    sent = [first] + [rest[2 + n * len(far_cores) :][: len(far_cores)] for n in range(kv_heads - 1)]
    crossed, windows = [], []
    for kv in all_kv:
        values = []
        for value, d in zip(sent[kv], far_cores):
            values.append(swapped(value, d))
        crossed.append(values)
        far = shifted(own[kv], 2)
        near = shifted(own[kv], 1)
        windows.append((far, near, own[kv]))
    here = rest[0]
    partner = swapped(rest[1], 1)
    dq_here, dq_partner, dq_crossed, totals = [], [], [], []
    for kv in all_kv:
        dq, (dfar, dnear, down) = group_grads(
            [here, partner] + crossed[kv], [kv, kv] + [0] * len(far_cores), *windows[kv]
        )
        dfar = shifted(dfar, -2)
        dnear = shifted(dnear, -1)
        dq_here.append(dq[0])
        dq_partner.append(dq[1])
        values = []
        for value, d in zip(dq[2:], far_cores):
            values.append(swapped(value, d))
        dq_crossed.append(values)
        totals.append((down, dfar, dnear))
    dq_partner = swapped(jnp.concatenate(dq_partner, axis=0), 1)
    values = dq_here + [dq_partner] + sum(dq_crossed, [])
    parts = [[(kv, 0)] for kv in all_kv] + [[(kv, 1) for kv in all_kv]]
    parts += [[(kv, d)] for kv in all_kv for d in far_cores]
    return finish(values, parts, totals)


def solution(mesh):
    return jax.shard_map(
        shards,
        mesh=mesh,
        in_specs=(
            P(("inner", "outer", "head"), None, None),
            P(("inner", "outer"), "head", None),
            P(("inner", "outer"), "head", None),
            P(("inner", "outer", "head"), None, None),
        ),
        out_specs=(
            P(("inner", "outer", "head"), None, None),
            P(("inner", "outer"), "head", None),
            P(("inner", "outer"), "head", None),
        ),
        check_vma=False,
    )
```

```python
import functools
import math

import jax
import jax.numpy as jnp
from jax import lax
from jax.experimental import pallas as pl
from jax.experimental.pallas import tpu as pltpu
from jax.sharding import PartitionSpec as P


NT = (((1,), (1,)), ((), ()))
SEQ = ("inner", "outer")
NEVER = 1e30
BLOCK = 256
VMEM = pl.BlockSpec(memory_space=pltpu.VMEM)
HBM = pl.BlockSpec(memory_space=pltpu.HBM)


def shifted(value, by):
    peers = lax.axis_size(SEQ)
    pairs = [(i, (i + by) % peers) for i in range(peers)]
    return lax.ppermute(value, SEQ, pairs)


def swapped(value, distance):
    peers = lax.axis_size("head")
    return lax.ppermute(value, "head", [(i, i ^ distance) for i in range(peers)])


def in_hbm(value):
    return pltpu.with_memory_space_constraint(value, pltpu.HBM)


def pack_copies(parts, sources, outs, sem, kv_heads):
    me = lax.axis_index("head")
    copies = []
    for out, part in zip(outs, parts):
        for n, (kv, distance) in enumerate(part):
            place = (me ^ distance) * kv_heads + kv
            for which, source in enumerate(sources):
                copies.append(
                    pltpu.make_async_copy(source.at[:, place], out.at[n, which], sem.at[len(copies)])
                )
    return copies


def pack_kernel(parts, kv_heads, q_ref, do_ref, *refs):
    copies = pack_copies(parts, (q_ref, do_ref), refs[:-1], refs[-1], kv_heads)
    for copy in copies:
        copy.start()
    for copy in copies:
        copy.wait()


def first_kernel(parts, kv_heads, key_ref, value_ref, q_ref, do_ref, *refs):
    own_refs, outs = refs[:kv_heads], refs[kv_heads:-4]
    narrow, wide, own_sem, sem = refs[-4:]
    loads = [
        pltpu.make_async_copy(source, narrow.at[which], own_sem.at[which])
        for which, source in enumerate((key_ref, value_ref))
    ]
    copies = pack_copies(parts, (q_ref, do_ref), outs, sem, kv_heads)
    for copy in loads + copies:
        copy.start()
    tok_rows = own_refs[0].shape[1]
    for which, load in enumerate(loads):
        load.wait()
        wide[which] = narrow[which].astype(jnp.float32)
        for kv in range(kv_heads):
            rows = wide[which, pl.ds(kv, tok_rows, stride=kv_heads), :]
            own_refs[kv][which] = rows.astype(own_refs[kv].dtype)
    for copy in copies:
        copy.wait()


def pack(queries, grad_out, parts, kv_heads):
    part_rows, _, group, width = queries.shape
    return pl.pallas_call(
        functools.partial(pack_kernel, parts, kv_heads),
        in_specs=[HBM, HBM],
        out_specs=[VMEM] * len(parts),
        out_shape=[
            pltpu.VMEM((len(part), 2, part_rows, group, width), queries.dtype) for part in parts
        ],
        scratch_shapes=[pltpu.SemaphoreType.DMA((2 * sum(len(part) for part in parts),))],
        compiler_params=pltpu.CompilerParams(vmem_limit_bytes=16 * 2**20),
        name="pack",
    )(in_hbm(queries), in_hbm(grad_out))


def pack_first(keys, values, queries, grad_out, parts):
    tok_rows, kv_heads, width = keys.shape
    part_rows, _, group, _ = queries.shape
    outs = pl.pallas_call(
        functools.partial(first_kernel, parts, kv_heads),
        in_specs=[HBM] * 4,
        out_specs=[VMEM] * (len(parts) + kv_heads),
        out_shape=[pltpu.VMEM((2, tok_rows, width), keys.dtype)] * kv_heads
        + [pltpu.VMEM((len(part), 2, part_rows, group, width), queries.dtype) for part in parts],
        scratch_shapes=[
            pltpu.VMEM((2, tok_rows * kv_heads, width), keys.dtype),
            pltpu.VMEM((2, tok_rows * kv_heads, width), jnp.float32),
            pltpu.SemaphoreType.DMA((2,)),
            pltpu.SemaphoreType.DMA((2 * sum(len(part) for part in parts),)),
        ],
        compiler_params=pltpu.CompilerParams(vmem_limit_bytes=16 * 2**20),
        name="first",
    )(
        in_hbm(keys.reshape(tok_rows * kv_heads, width)),
        in_hbm(values.reshape(tok_rows * kv_heads, width)),
        in_hbm(queries),
        in_hbm(grad_out),
    )
    return outs[:kv_heads], outs[kv_heads:]


def finish_kernel(parts, heads, *refs):
    values, totals = refs[: len(parts)], refs[len(parts) : len(parts) + 3 * heads]
    dq_ref, dk_ref, dv_ref, wide, narrow, sem = refs[len(parts) + 3 * heads :]
    me = lax.axis_index("head")
    copies = []
    for value, part in zip(values, parts):
        for n, (kv, distance) in enumerate(part):
            place = (me ^ distance) * heads + kv
            copies.append(
                pltpu.make_async_copy(value.at[n], dq_ref.at[:, place], sem.at[len(copies)])
            )
    for copy in copies:
        copy.start()
    tok_rows = totals[0].shape[1]
    for which, out in enumerate((dk_ref, dv_ref)):
        for kv in range(heads):
            own, far, near = totals[3 * kv : 3 * kv + 3]
            total = own[which] + far[which].astype(jnp.float32) + near[which].astype(jnp.float32)
            wide[which, pl.ds(kv, tok_rows, stride=heads), :] = total
        narrow[which] = wide[which].astype(narrow.dtype)
        copies.append(pltpu.make_async_copy(narrow.at[which], out, sem.at[len(copies)]))
        copies[-1].start()
    for copy in copies:
        copy.wait()


def finish(values, parts, totals):
    _, part_rows, group, width = values[0].shape
    heads = len(totals)
    tok_rows = totals[0][0].shape[1]
    places = sum(len(part) for part in parts)
    dq, dk, dv = pl.pallas_call(
        functools.partial(finish_kernel, parts, heads),
        in_specs=[VMEM] * (len(values) + 3 * heads),
        out_specs=[HBM] * 3,
        out_shape=[
            jax.ShapeDtypeStruct((part_rows, places, group, width), jnp.bfloat16),
            jax.ShapeDtypeStruct((tok_rows * heads, width), jnp.bfloat16),
            jax.ShapeDtypeStruct((tok_rows * heads, width), jnp.bfloat16),
        ],
        scratch_shapes=[
            pltpu.VMEM((2, tok_rows * heads, width), jnp.float32),
            pltpu.VMEM((2, tok_rows * heads, width), jnp.bfloat16),
            pltpu.SemaphoreType.DMA((places + 2,)),
        ],
        compiler_params=pltpu.CompilerParams(vmem_limit_bytes=16 * 2**20),
        name="finish",
    )(*values, *(term for total in totals for term in total))
    return (
        dq.reshape(part_rows, places * group, width),
        dk.reshape(tok_rows, heads, width),
        dv.reshape(tok_rows, heads, width),
    )


def grads_kernel(where, distances, fresh, last, *refs):
    count = len(distances)
    pair_refs, windows = refs[:count], refs[count : count + 3]
    spent = count + 3 + (0 if fresh else 1)
    old_ref = None if fresh else refs[count + 3]
    dq_refs = refs[spent : spent + count]
    sum_refs = refs[spent + count : -2]
    acc, kt = refs[-2:]
    _, part_rows, group, width = pair_refs[0].shape[1:]
    rows = part_rows * group
    block_rows = min(rows, BLOCK)
    scale = width ** (-0.5)
    to_exp2 = scale * math.log2(math.e)
    me = lax.axis_index("head")
    block = lax.axis_index(SEQ)
    bias = (
        jnp.where(block < 2, NEVER, 0.0).astype(jnp.float32),
        jnp.where(block < 1, NEVER, 0.0).astype(jnp.float32),
        0.0,
    )
    for j, window in enumerate(windows):
        kt[j] = window[0].T
    tokens = block_rows // group
    pieces = [(n, t) for n in range(count) for t in range(0, part_rows, tokens)]

    def part(piece, which):
        n, t = piece
        return pair_refs[n][where[n], which, t : t + tokens].reshape(block_rows, width)

    def scored(piece):
        n, t = piece
        q = part(piece, 0)
        first = (me ^ distances[n]) * rows + t * group
        scores, tops = [], []
        for j, window in enumerate(windows):
            s = lax.dot_general(window[0], q, NT, preferred_element_type=jnp.float32)
            if j == 2:
                token = (lax.broadcasted_iota(jnp.int32, (1, block_rows), 1) + first) // group
                key = lax.broadcasted_iota(jnp.int32, s.shape, 0)
                s = jnp.where(key <= token, s, -jnp.inf)
            scores.append(s)
            tops.append(jnp.max(s, axis=0, keepdims=True) - bias[j])
        return scores, jnp.maximum(jnp.maximum(tops[0], tops[1]), tops[2]) * to_exp2

    ahead = scored(pieces[0])
    for step, piece in enumerate(pieces):
        scores, top = ahead
        q, do = part(piece, 0), part(piece, 1)
        weights, dprobs, total, dtotal = [], [], 0.0, 0.0
        for j, window in enumerate(windows):
            e = jnp.exp2(scores[j] * to_exp2 - (top + bias[j]))
            dp = lax.dot_general(window[1], do, NT, preferred_element_type=jnp.float32)
            total = total + jnp.sum(e, axis=0, keepdims=True)
            dtotal = dtotal + jnp.sum(e * dp, axis=0, keepdims=True)
            weights.append(e)
            dprobs.append(dp)
        if step + 1 < len(pieces):
            ahead = scored(pieces[step + 1])
        inverse = 1.0 / total
        delta = dtotal * inverse
        dqt = 0.0
        for j in range(3):
            p = weights[j] * inverse
            ds = (p * (dprobs[j] - delta)).astype(jnp.bfloat16)
            dv = jnp.dot(p.astype(jnp.bfloat16), do, preferred_element_type=jnp.float32)
            dk = jnp.dot(ds, q, preferred_element_type=jnp.float32)
            if step == 0:
                if not fresh:
                    dk, dv = old_ref[j, 0] + dk, old_ref[j, 1] + dv
                acc[j, 0], acc[j, 1] = dk, dv
            else:
                acc[j, 0] += dk
                acc[j, 1] += dv
            dqt = dqt + jnp.dot(kt[j], ds, preferred_element_type=jnp.float32)
        n, t = piece
        dq = (dqt * scale).T.astype(jnp.bfloat16)
        dq_refs[n][0, t : t + tokens] = dq.reshape(tokens, group, width)
    if last:
        for j, out in enumerate(sum_refs):
            out[0] = (acc[j, 0] * scale).astype(out.dtype)
            out[1] = acc[j, 1].astype(out.dtype)
    else:
        sum_refs[0][...] = acc[...]


def group_grads(pairs, where, distances, window, sums, last):
    count = len(pairs)
    _, _, part_rows, group, width = pairs[0].shape
    tok_rows = window[2].shape[1]
    rows = part_rows * group
    cells = count * rows * 3 * tok_rows
    shape = (2, tok_rows, width)
    if last:
        kinds = [pltpu.VMEM(shape, jnp.bfloat16)] * 2 + [pltpu.VMEM(shape, jnp.float32)]
    else:
        kinds = [pltpu.VMEM((3, *shape), jnp.float32)]
    old = [] if sums is None else [sums]
    outs = pl.pallas_call(
        functools.partial(grads_kernel, where, distances, sums is None, last),
        in_specs=[VMEM] * (count + 3 + len(old)),
        out_specs=[VMEM] * (count + len(kinds)),
        out_shape=[pltpu.VMEM((1, part_rows, group, width), jnp.bfloat16)] * count + kinds,
        scratch_shapes=[
            pltpu.VMEM((3, *shape), jnp.float32),
            pltpu.VMEM((3, width, tok_rows), jnp.bfloat16),
        ],
        compiler_params=pltpu.CompilerParams(vmem_limit_bytes=32 * 2**20),
        cost_estimate=pl.CostEstimate(
            flops=10 * cells * width, bytes_accessed=6 * count * rows * width, transcendentals=cells
        ),
        name="grads",
    )(*pairs, *window, *old)
    return outs[:count], outs[count:]


def shards(queries, key_vector_rows, value_vector_rows, grad_out):
    part_rows, heads, width = queries.shape
    kv_heads = key_vector_rows.shape[1]
    peers = lax.axis_size("head")
    group = heads // (peers * kv_heads)
    places = peers * kv_heads
    queries = queries.reshape(part_rows, places, group, width)
    grad_out = grad_out.reshape(part_rows, places, group, width)
    far_cores = list(range(2, peers))
    all_kv = list(range(kv_heads))

    own, first = pack_first(
        key_vector_rows, value_vector_rows, queries, grad_out, [[(0, d)] for d in far_cores]
    )
    rest = pack(
        queries,
        grad_out,
        [[(kv, 0) for kv in all_kv], [(kv, 1) for kv in all_kv]]
        + [[(kv, d)] for kv in all_kv[1:] for d in far_cores],
        kv_heads,
    )
    sent = [first] + [rest[2 + n * len(far_cores) :][: len(far_cores)] for n in range(kv_heads - 1)]
    crossed, windows = [], []
    for kv in all_kv:
        values = []
        for value, d in zip(sent[kv], far_cores):
            values.append(swapped(value, d))
        crossed.append(values)
        far = shifted(own[kv], 2)
        near = shifted(own[kv], 1)
        windows.append((far, near, own[kv]))
    here = rest[0]
    partner = swapped(rest[1], 1)
    dq, totals = {}, []
    for kv in all_kv:
        final = kv == all_kv[-1]
        turns = [[0, 1]] + [[d] for d in far_cores]
        sums = None
        for turn in turns:
            values = {0: here, 1: partner, **dict(zip(far_cores, crossed[kv]))}
            made, sums = group_grads(
                [values[d] for d in turn],
                [kv if d < 2 else 0 for d in turn],
                turn,
                windows[kv],
                None if sums is None else sums[0],
                turn is turns[-1],
            )
            for d, value in zip(turn, made):
                if d >= 2:
                    value = swapped(value, d)
                dq[kv, d] = value
        dfar = shifted(sums[0], -2)
        dnear = shifted(sums[1], -1)
        totals.append((sums[2], dfar, dnear))
    dq_partner = swapped(jnp.concatenate([dq[kv, 1] for kv in all_kv], axis=0), 1)
    parts = [[(kv, 0)] for kv in all_kv] + [[(kv, 1) for kv in all_kv]]
    parts += [[(kv, d)] for kv in all_kv for d in far_cores]
    values = [dq[part[0]] if len(part) == 1 else dq_partner for part in parts]
    return finish(values, parts, totals)


def solution(mesh):
    return jax.shard_map(
        shards,
        mesh=mesh,
        in_specs=(
            P(("inner", "outer", "head"), None, None),
            P(("inner", "outer"), "head", None),
            P(("inner", "outer"), "head", None),
            P(("inner", "outer", "head"), None, None),
        ),
        out_specs=(
            P(("inner", "outer", "head"), None, None),
            P(("inner", "outer"), "head", None),
            P(("inner", "outer"), "head", None),
        ),
        check_vma=False,
    )
```

```python
import functools
import math

import jax
import jax.numpy as jnp
from jax import lax
from jax.experimental import pallas as pl
from jax.experimental.pallas import tpu as pltpu
from jax.sharding import PartitionSpec as P


NT = (((1,), (1,)), ((), ()))
SEQ = ("inner", "outer")
NEVER = 1e30
BLOCK = 256
VMEM = pl.BlockSpec(memory_space=pltpu.VMEM)
HBM = pl.BlockSpec(memory_space=pltpu.HBM)


def shifted(value, by):
    peers = lax.axis_size(SEQ)
    pairs = [(i, (i + by) % peers) for i in range(peers)]
    return lax.ppermute(value, SEQ, pairs)


def swapped(value, distance):
    peers = lax.axis_size("head")
    return lax.ppermute(value, "head", [(i, i ^ distance) for i in range(peers)])


def in_hbm(value):
    return pltpu.with_memory_space_constraint(value, pltpu.HBM)


def pack_copies(parts, sources, outs, sem, kv_heads):
    me = lax.axis_index("head")
    copies = []
    for out, part in zip(outs, parts):
        for n, (kv, distance) in enumerate(part):
            place = (me ^ distance) * kv_heads + kv
            for which, source in enumerate(sources):
                copies.append(
                    pltpu.make_async_copy(source.at[:, place], out.at[n, which], sem.at[len(copies)])
                )
    return copies


def pack_kernel(parts, kv_heads, q_ref, do_ref, *refs):
    copies = pack_copies(parts, (q_ref, do_ref), refs[:-1], refs[-1], kv_heads)
    for copy in copies:
        copy.start()
    for copy in copies:
        copy.wait()


def first_kernel(parts, kv_heads, key_ref, value_ref, q_ref, do_ref, *refs):
    own_refs, outs = refs[:kv_heads], refs[kv_heads:-4]
    narrow, wide, own_sem, sem = refs[-4:]
    loads = [
        pltpu.make_async_copy(source, narrow.at[which], own_sem.at[which])
        for which, source in enumerate((key_ref, value_ref))
    ]
    copies = pack_copies(parts, (q_ref, do_ref), outs, sem, kv_heads)
    for copy in loads + copies:
        copy.start()
    tok_rows = own_refs[0].shape[1]
    for which, load in enumerate(loads):
        load.wait()
        wide[which] = narrow[which].astype(jnp.float32)
        for kv in range(kv_heads):
            rows = wide[which, pl.ds(kv, tok_rows, stride=kv_heads), :]
            own_refs[kv][which] = rows.astype(own_refs[kv].dtype)
    for copy in copies:
        copy.wait()


def pack(queries, grad_out, parts, kv_heads):
    part_rows, _, group, width = queries.shape
    return pl.pallas_call(
        functools.partial(pack_kernel, parts, kv_heads),
        in_specs=[HBM, HBM],
        out_specs=[VMEM] * len(parts),
        out_shape=[
            pltpu.VMEM((len(part), 2, part_rows, group, width), queries.dtype) for part in parts
        ],
        scratch_shapes=[pltpu.SemaphoreType.DMA((2 * sum(len(part) for part in parts),))],
        compiler_params=pltpu.CompilerParams(vmem_limit_bytes=16 * 2**20),
        name="pack",
    )(in_hbm(queries), in_hbm(grad_out))


def pack_first(keys, values, queries, grad_out, parts):
    tok_rows, kv_heads, width = keys.shape
    part_rows, _, group, _ = queries.shape
    outs = pl.pallas_call(
        functools.partial(first_kernel, parts, kv_heads),
        in_specs=[HBM] * 4,
        out_specs=[VMEM] * (len(parts) + kv_heads),
        out_shape=[pltpu.VMEM((2, tok_rows, width), keys.dtype)] * kv_heads
        + [pltpu.VMEM((len(part), 2, part_rows, group, width), queries.dtype) for part in parts],
        scratch_shapes=[
            pltpu.VMEM((2, tok_rows * kv_heads, width), keys.dtype),
            pltpu.VMEM((2, tok_rows * kv_heads, width), jnp.float32),
            pltpu.SemaphoreType.DMA((2,)),
            pltpu.SemaphoreType.DMA((2 * sum(len(part) for part in parts),)),
        ],
        compiler_params=pltpu.CompilerParams(vmem_limit_bytes=16 * 2**20),
        name="first",
    )(
        in_hbm(keys.reshape(tok_rows * kv_heads, width)),
        in_hbm(values.reshape(tok_rows * kv_heads, width)),
        in_hbm(queries),
        in_hbm(grad_out),
    )
    return outs[:kv_heads], outs[kv_heads:]


def place_copies(values, parts, out_ref, sem, heads):
    me = lax.axis_index("head")
    copies = []
    for value, part in zip(values, parts):
        for n, (kv, distance) in enumerate(part):
            place = (me ^ distance) * heads + kv
            copies.append(
                pltpu.make_async_copy(value.at[n], out_ref.at[:, place], sem.at[len(copies)])
            )
    return copies


def store_kernel(parts, heads, *refs):
    copies = place_copies(refs[:-2], parts, refs[-2], refs[-1], heads)
    for copy in copies:
        copy.start()
    for copy in copies:
        copy.wait()


def store(values, parts, places, heads):
    _, part_rows, group, width = values[0].shape
    return pl.pallas_call(
        functools.partial(store_kernel, parts, heads),
        in_specs=[VMEM] * len(values),
        out_specs=HBM,
        out_shape=pltpu.HBM((part_rows, places, group, width), jnp.bfloat16),
        scratch_shapes=[pltpu.SemaphoreType.DMA((sum(len(part) for part in parts),))],
        compiler_params=pltpu.CompilerParams(vmem_limit_bytes=16 * 2**20),
        name="store",
    )(*values)


def finish_kernel(parts, heads, old_ref, *refs):
    values, totals = refs[: len(parts)], refs[len(parts) : len(parts) + 3 * heads]
    dq_ref, dk_ref, dv_ref, wide, narrow, sem = refs[len(parts) + 3 * heads :]
    copies = place_copies(values, parts, dq_ref, sem, heads)
    for copy in copies:
        copy.start()
    tok_rows = totals[0].shape[1]
    for which, out in enumerate((dk_ref, dv_ref)):
        for kv in range(heads):
            own, far, near = totals[3 * kv : 3 * kv + 3]
            total = own[which] + far[which].astype(jnp.float32) + near[which].astype(jnp.float32)
            wide[which, pl.ds(kv, tok_rows, stride=heads), :] = total
        narrow[which] = wide[which].astype(narrow.dtype)
        copies.append(pltpu.make_async_copy(narrow.at[which], out, sem.at[len(copies)]))
        copies[-1].start()
    for copy in copies:
        copy.wait()


def finish(stored, values, parts, totals):
    part_rows, places, group, width = stored.shape
    heads = len(totals)
    tok_rows = totals[0][0].shape[1]
    dq, dk, dv = pl.pallas_call(
        functools.partial(finish_kernel, parts, heads),
        in_specs=[HBM] + [VMEM] * (len(values) + 3 * heads),
        out_specs=[HBM] * 3,
        out_shape=[
            pltpu.HBM((part_rows, places, group, width), jnp.bfloat16),
            pltpu.HBM((tok_rows * heads, width), jnp.bfloat16),
            pltpu.HBM((tok_rows * heads, width), jnp.bfloat16),
        ],
        scratch_shapes=[
            pltpu.VMEM((2, tok_rows * heads, width), jnp.float32),
            pltpu.VMEM((2, tok_rows * heads, width), jnp.bfloat16),
            pltpu.SemaphoreType.DMA((sum(len(part) for part in parts) + 2,)),
        ],
        input_output_aliases={0: 0},
        compiler_params=pltpu.CompilerParams(vmem_limit_bytes=16 * 2**20),
        name="finish",
    )(stored, *values, *(term for total in totals for term in total))
    return (
        dq.reshape(part_rows, places * group, width),
        dk.reshape(tok_rows, heads, width),
        dv.reshape(tok_rows, heads, width),
    )


def grads_kernel(where, distances, fresh, last, *refs):
    count = len(distances)
    pair_refs, windows = refs[:count], refs[count : count + 3]
    spent = count + 3 + (0 if fresh else 1)
    old_ref = None if fresh else refs[count + 3]
    dq_refs = refs[spent : spent + count]
    sum_refs = refs[spent + count : -2]
    acc, kt = refs[-2:]
    _, part_rows, group, width = pair_refs[0].shape[1:]
    rows = part_rows * group
    block_rows = min(rows, BLOCK)
    scale = width ** (-0.5)
    to_exp2 = scale * math.log2(math.e)
    me = lax.axis_index("head")
    block = lax.axis_index(SEQ)
    bias = (
        jnp.where(block < 2, NEVER, 0.0).astype(jnp.float32),
        jnp.where(block < 1, NEVER, 0.0).astype(jnp.float32),
        0.0,
    )
    for j, window in enumerate(windows):
        kt[j] = window[0].T
    tokens = block_rows // group
    pieces = [(n, t) for n in range(count) for t in range(0, part_rows, tokens)]

    def part(piece, which):
        n, t = piece
        return pair_refs[n][where[n], which, t : t + tokens].reshape(block_rows, width)

    def scored(piece):
        n, t = piece
        q = part(piece, 0)
        first = (me ^ distances[n]) * rows + t * group
        scores, tops = [], []
        for j, window in enumerate(windows):
            s = lax.dot_general(window[0], q, NT, preferred_element_type=jnp.float32)
            if j == 2:
                token = (lax.broadcasted_iota(jnp.int32, (1, block_rows), 1) + first) // group
                key = lax.broadcasted_iota(jnp.int32, s.shape, 0)
                s = jnp.where(key <= token, s, -jnp.inf)
            scores.append(s)
            tops.append(jnp.max(s, axis=0, keepdims=True) - bias[j])
        return scores, jnp.maximum(jnp.maximum(tops[0], tops[1]), tops[2]) * to_exp2

    ahead = scored(pieces[0])
    for step, piece in enumerate(pieces):
        scores, top = ahead
        q, do = part(piece, 0), part(piece, 1)
        weights, dprobs, total, dtotal = [], [], 0.0, 0.0
        for j, window in enumerate(windows):
            e = jnp.exp2(scores[j] * to_exp2 - (top + bias[j]))
            dp = lax.dot_general(window[1], do, NT, preferred_element_type=jnp.float32)
            total = total + jnp.sum(e, axis=0, keepdims=True)
            dtotal = dtotal + jnp.sum(e * dp, axis=0, keepdims=True)
            weights.append(e)
            dprobs.append(dp)
        if step + 1 < len(pieces):
            ahead = scored(pieces[step + 1])
        inverse = 1.0 / total
        delta = dtotal * inverse
        dqt = 0.0
        for j in range(3):
            p = weights[j] * inverse
            ds = (p * (dprobs[j] - delta)).astype(jnp.bfloat16)
            dv = jnp.dot(p.astype(jnp.bfloat16), do, preferred_element_type=jnp.float32)
            dk = jnp.dot(ds, q, preferred_element_type=jnp.float32)
            if step == 0:
                if not fresh:
                    dk, dv = old_ref[j, 0] + dk, old_ref[j, 1] + dv
                acc[j, 0], acc[j, 1] = dk, dv
            else:
                acc[j, 0] += dk
                acc[j, 1] += dv
            dqt = dqt + jnp.dot(kt[j], ds, preferred_element_type=jnp.float32)
        n, t = piece
        dq = (dqt * scale).T.astype(jnp.bfloat16)
        dq_refs[n][0, t : t + tokens] = dq.reshape(tokens, group, width)
    if last:
        for j, out in enumerate(sum_refs):
            out[0] = (acc[j, 0] * scale).astype(out.dtype)
            out[1] = acc[j, 1].astype(out.dtype)
    else:
        sum_refs[0][...] = acc[...]


def group_grads(pairs, where, distances, window, sums, last):
    count = len(pairs)
    _, _, part_rows, group, width = pairs[0].shape
    tok_rows = window[2].shape[1]
    rows = part_rows * group
    cells = count * rows * 3 * tok_rows
    shape = (2, tok_rows, width)
    if last:
        kinds = [pltpu.VMEM(shape, jnp.bfloat16)] * 2 + [pltpu.VMEM(shape, jnp.float32)]
    else:
        kinds = [pltpu.VMEM((3, *shape), jnp.float32)]
    old = [] if sums is None else [sums]
    outs = pl.pallas_call(
        functools.partial(grads_kernel, where, distances, sums is None, last),
        in_specs=[VMEM] * (count + 3 + len(old)),
        out_specs=[VMEM] * (count + len(kinds)),
        out_shape=[pltpu.VMEM((1, part_rows, group, width), jnp.bfloat16)] * count + kinds,
        scratch_shapes=[
            pltpu.VMEM((3, *shape), jnp.float32),
            pltpu.VMEM((3, width, tok_rows), jnp.bfloat16),
        ],
        compiler_params=pltpu.CompilerParams(vmem_limit_bytes=32 * 2**20),
        cost_estimate=pl.CostEstimate(
            flops=10 * cells * width, bytes_accessed=6 * count * rows * width, transcendentals=cells
        ),
        name="grads",
    )(*pairs, *window, *old)
    return outs[:count], outs[count:]


def shards(queries, key_vector_rows, value_vector_rows, grad_out):
    part_rows, heads, width = queries.shape
    kv_heads = key_vector_rows.shape[1]
    peers = lax.axis_size("head")
    group = heads // (peers * kv_heads)
    places = peers * kv_heads
    queries = queries.reshape(part_rows, places, group, width)
    grad_out = grad_out.reshape(part_rows, places, group, width)
    far_cores = list(range(2, peers))
    all_kv = list(range(kv_heads))

    own, first = pack_first(
        key_vector_rows, value_vector_rows, queries, grad_out, [[(0, d)] for d in far_cores]
    )
    rest = pack(
        queries,
        grad_out,
        [[(kv, 0) for kv in all_kv], [(kv, 1) for kv in all_kv]]
        + [[(kv, d)] for kv in all_kv[1:] for d in far_cores],
        kv_heads,
    )
    sent = [first] + [rest[2 + n * len(far_cores) :][: len(far_cores)] for n in range(kv_heads - 1)]
    crossed, windows = [], []
    for kv in all_kv:
        values = []
        for value, d in zip(sent[kv], far_cores):
            values.append(swapped(value, d))
        crossed.append(values)
        far = shifted(own[kv], 2)
        near = shifted(own[kv], 1)
        windows.append((far, near, own[kv]))
    here = rest[0]
    partner = swapped(rest[1], 1)
    dq, totals = {}, []
    for kv in all_kv:
        final = kv == all_kv[-1]
        turns = [[0, 1]] + [[d] for d in far_cores]
        sums = None
        for turn in turns:
            values = {0: here, 1: partner, **dict(zip(far_cores, crossed[kv]))}
            made, sums = group_grads(
                [values[d] for d in turn],
                [kv if d < 2 else 0 for d in turn],
                turn,
                windows[kv],
                None if sums is None else sums[0],
                turn is turns[-1],
            )
            for d, value in zip(turn, made):
                if d >= 2:
                    value = swapped(value, d)
                dq[kv, d] = value
        dfar = shifted(sums[0], -2)
        dnear = shifted(sums[1], -1)
        totals.append((sums[2], dfar, dnear))
    dq_partner = swapped(jnp.concatenate([dq[kv, 1] for kv in all_kv], axis=0), 1)
    early = [[(kv, 0)] for kv in all_kv] + [[(kv, 1) for kv in all_kv]]
    early += [[(kv, d)] for kv in all_kv[:-1] for d in far_cores]
    values = [dq[part[0]] if len(part) == 1 else dq_partner for part in early]
    stored = store(values, early, places, kv_heads)
    late = [(all_kv[-1], d) for d in far_cores]
    return finish(stored, [dq[key] for key in late], [[key] for key in late], totals)


def solution(mesh):
    return jax.shard_map(
        shards,
        mesh=mesh,
        in_specs=(
            P(("inner", "outer", "head"), None, None),
            P(("inner", "outer"), "head", None),
            P(("inner", "outer"), "head", None),
            P(("inner", "outer", "head"), None, None),
        ),
        out_specs=(
            P(("inner", "outer", "head"), None, None),
            P(("inner", "outer"), "head", None),
            P(("inner", "outer"), "head", None),
        ),
        check_vma=False,
    )
```

```python
import functools
import math

import jax
import jax.numpy as jnp
from jax import lax
from jax.experimental import pallas as pl
from jax.experimental.pallas import tpu as pltpu
from jax.sharding import PartitionSpec as P


NT = (((1,), (1,)), ((), ()))
SEQ = ("inner", "outer")
NEVER = 1e30
BLOCK = 256
VMEM = pl.BlockSpec(memory_space=pltpu.VMEM)
HBM = pl.BlockSpec(memory_space=pltpu.HBM)


def shifted(value, by):
    peers = lax.axis_size(SEQ)
    pairs = [(i, (i + by) % peers) for i in range(peers)]
    return lax.ppermute(value, SEQ, pairs)


def swapped(value, distance):
    peers = lax.axis_size("head")
    return lax.ppermute(value, "head", [(i, i ^ distance) for i in range(peers)])


def in_hbm(value):
    return pltpu.with_memory_space_constraint(value, pltpu.HBM)


def pack_copies(parts, sources, outs, sem, kv_heads):
    me = lax.axis_index("head")
    copies = []
    for out, part in zip(outs, parts):
        for n, (kv, distance) in enumerate(part):
            place = (me ^ distance) * kv_heads + kv
            for which, source in enumerate(sources):
                copies.append(
                    pltpu.make_async_copy(source.at[:, place], out.at[n, which], sem.at[len(copies)])
                )
    return copies


def pack_kernel(parts, kv_heads, q_ref, do_ref, *refs):
    copies = pack_copies(parts, (q_ref, do_ref), refs[:-1], refs[-1], kv_heads)
    for copy in copies:
        copy.start()
    for copy in copies:
        copy.wait()


def first_kernel(parts, kv_heads, key_ref, value_ref, q_ref, do_ref, *refs):
    own_refs, outs = refs[:kv_heads], refs[kv_heads:-4]
    narrow, wide, own_sem, sem = refs[-4:]
    loads = [
        pltpu.make_async_copy(source, narrow.at[which], own_sem.at[which])
        for which, source in enumerate((key_ref, value_ref))
    ]
    copies = pack_copies(parts, (q_ref, do_ref), outs, sem, kv_heads)
    for copy in loads + copies:
        copy.start()
    tok_rows = own_refs[0].shape[1]
    for which, load in enumerate(loads):
        load.wait()
        wide[which] = narrow[which].astype(jnp.float32)
        for kv in range(kv_heads):
            rows = wide[which, pl.ds(kv, tok_rows, stride=kv_heads), :]
            own_refs[kv][which] = rows.astype(own_refs[kv].dtype)
    for copy in copies:
        copy.wait()


def pack(queries, grad_out, parts, kv_heads):
    part_rows, _, group, width = queries.shape
    return pl.pallas_call(
        functools.partial(pack_kernel, parts, kv_heads),
        in_specs=[HBM, HBM],
        out_specs=[VMEM] * len(parts),
        out_shape=[
            pltpu.VMEM((len(part), 2, part_rows, group, width), queries.dtype) for part in parts
        ],
        scratch_shapes=[pltpu.SemaphoreType.DMA((2 * sum(len(part) for part in parts),))],
        compiler_params=pltpu.CompilerParams(vmem_limit_bytes=16 * 2**20),
        name="pack",
    )(in_hbm(queries), in_hbm(grad_out))


def pack_first(keys, values, queries, grad_out, parts):
    tok_rows, kv_heads, width = keys.shape
    part_rows, _, group, _ = queries.shape
    outs = pl.pallas_call(
        functools.partial(first_kernel, parts, kv_heads),
        in_specs=[HBM] * 4,
        out_specs=[VMEM] * (len(parts) + kv_heads),
        out_shape=[pltpu.VMEM((2, tok_rows, width), keys.dtype)] * kv_heads
        + [pltpu.VMEM((len(part), 2, part_rows, group, width), queries.dtype) for part in parts],
        scratch_shapes=[
            pltpu.VMEM((2, tok_rows * kv_heads, width), keys.dtype),
            pltpu.VMEM((2, tok_rows * kv_heads, width), jnp.float32),
            pltpu.SemaphoreType.DMA((2,)),
            pltpu.SemaphoreType.DMA((2 * sum(len(part) for part in parts),)),
        ],
        compiler_params=pltpu.CompilerParams(vmem_limit_bytes=16 * 2**20),
        name="first",
    )(
        in_hbm(keys.reshape(tok_rows * kv_heads, width)),
        in_hbm(values.reshape(tok_rows * kv_heads, width)),
        in_hbm(queries),
        in_hbm(grad_out),
    )
    return outs[:kv_heads], outs[kv_heads:]


def place_copies(values, parts, out_ref, sem, heads):
    me = lax.axis_index("head")
    copies = []
    for value, part in zip(values, parts):
        for n, (kv, distance) in enumerate(part):
            place = (me ^ distance) * heads + kv
            copies.append(
                pltpu.make_async_copy(value.at[n], out_ref.at[:, place], sem.at[len(copies)])
            )
    return copies


def store_kernel(parts, heads, *refs):
    copies = place_copies(refs[:-2], parts, refs[-2], refs[-1], heads)
    for copy in copies:
        copy.start()
    for copy in copies:
        copy.wait()


def store(values, parts, places, heads):
    _, part_rows, group, width = values[0].shape
    return pl.pallas_call(
        functools.partial(store_kernel, parts, heads),
        in_specs=[VMEM] * len(values),
        out_specs=HBM,
        out_shape=pltpu.HBM((part_rows, places, group, width), jnp.bfloat16),
        scratch_shapes=[pltpu.SemaphoreType.DMA((sum(len(part) for part in parts),))],
        compiler_params=pltpu.CompilerParams(vmem_limit_bytes=16 * 2**20),
        name="store",
    )(*values)


def finish_kernel(parts, heads, old_ref, *refs):
    values, totals = refs[: len(parts)], refs[len(parts) : len(parts) + 3 * heads]
    dq_ref, dk_ref, dv_ref, wide, narrow, sem = refs[len(parts) + 3 * heads :]
    copies = place_copies(values, parts, dq_ref, sem, heads)
    for copy in copies:
        copy.start()
    tok_rows = totals[0].shape[1]
    for which, out in enumerate((dk_ref, dv_ref)):
        for kv in range(heads):
            own, far, near = totals[3 * kv : 3 * kv + 3]
            total = own[which] + far[which].astype(jnp.float32) + near[which].astype(jnp.float32)
            wide[which, pl.ds(kv, tok_rows, stride=heads), :] = total
        narrow[which] = wide[which].astype(narrow.dtype)
        copies.append(pltpu.make_async_copy(narrow.at[which], out, sem.at[len(copies)]))
        copies[-1].start()
    for copy in copies:
        copy.wait()


def finish(stored, values, parts, totals):
    part_rows, places, group, width = stored.shape
    heads = len(totals)
    tok_rows = totals[0][0].shape[1]
    dq, dk, dv = pl.pallas_call(
        functools.partial(finish_kernel, parts, heads),
        in_specs=[HBM] + [VMEM] * (len(values) + 3 * heads),
        out_specs=[HBM] * 3,
        out_shape=[
            pltpu.HBM((part_rows, places, group, width), jnp.bfloat16),
            pltpu.HBM((tok_rows * heads, width), jnp.bfloat16),
            pltpu.HBM((tok_rows * heads, width), jnp.bfloat16),
        ],
        scratch_shapes=[
            pltpu.VMEM((2, tok_rows * heads, width), jnp.float32),
            pltpu.VMEM((2, tok_rows * heads, width), jnp.bfloat16),
            pltpu.SemaphoreType.DMA((sum(len(part) for part in parts) + 2,)),
        ],
        input_output_aliases={0: 0},
        compiler_params=pltpu.CompilerParams(vmem_limit_bytes=16 * 2**20),
        name="finish",
    )(stored, *values, *(term for total in totals for term in total))
    return (
        dq.reshape(part_rows, places * group, width),
        dk.reshape(tok_rows, heads, width),
        dv.reshape(tok_rows, heads, width),
    )


def grads_kernel(where, distances, fresh, last, *refs):
    count = len(distances)
    pair_refs, windows = refs[:count], refs[count : count + 3]
    spent = count + 3 + (0 if fresh else 1)
    old_ref = None if fresh else refs[count + 3]
    dq_refs = refs[spent : spent + count]
    sum_refs = refs[spent + count : -2]
    acc, kt = refs[-2:]
    _, part_rows, group, width = pair_refs[0].shape[1:]
    rows = part_rows * group
    block_rows = min(rows, BLOCK)
    scale = width ** (-0.5)
    to_exp2 = scale * math.log2(math.e)
    me = lax.axis_index("head")
    block = lax.axis_index(SEQ)
    bias = (
        jnp.where(block < 2, NEVER, 0.0).astype(jnp.float32),
        jnp.where(block < 1, NEVER, 0.0).astype(jnp.float32),
        0.0,
    )
    for j, window in enumerate(windows):
        kt[j] = window[0].T
    tokens = block_rows // group
    pieces = [(n, t) for n in range(count) for t in range(0, part_rows, tokens)]

    def part(piece, which):
        n, t = piece
        return pair_refs[n][where[n], which, t : t + tokens].reshape(block_rows, width)

    def value_dots(piece):
        do = part(piece, 1)
        return [
            lax.dot_general(window[1], do, NT, preferred_element_type=jnp.float32)
            for window in windows
        ]

    def scored(piece):
        n, t = piece
        q = part(piece, 0)
        first = (me ^ distances[n]) * rows + t * group
        scores, tops = [], []
        for j, window in enumerate(windows):
            s = lax.dot_general(window[0], q, NT, preferred_element_type=jnp.float32)
            if j == 2:
                token = (lax.broadcasted_iota(jnp.int32, (1, block_rows), 1) + first) // group
                key = lax.broadcasted_iota(jnp.int32, s.shape, 0)
                s = jnp.where(key <= token, s, -jnp.inf)
            scores.append(s)
            tops.append(jnp.max(s, axis=0, keepdims=True) - bias[j])
        dps = value_dots(piece) if count == 1 else None
        return scores, dps, jnp.maximum(jnp.maximum(tops[0], tops[1]), tops[2]) * to_exp2

    ahead = scored(pieces[0])
    for step, piece in enumerate(pieces):
        scores, dps, top = ahead
        q, do = part(piece, 0), part(piece, 1)
        weights, dprobs, total, dtotal = [], [], 0.0, 0.0
        for j, window in enumerate(windows):
            e = jnp.exp2(scores[j] * to_exp2 - (top + bias[j]))
            if dps is None:
                dp = lax.dot_general(window[1], do, NT, preferred_element_type=jnp.float32)
            else:
                dp = dps[j]
            total = total + jnp.sum(e, axis=0, keepdims=True)
            dtotal = dtotal + jnp.sum(e * dp, axis=0, keepdims=True)
            weights.append(e)
            dprobs.append(dp)
        if step + 1 < len(pieces):
            ahead = scored(pieces[step + 1])
        inverse = 1.0 / total
        delta = dtotal * inverse
        dqt = 0.0
        for j in range(3):
            p = weights[j] * inverse
            ds = (p * (dprobs[j] - delta)).astype(jnp.bfloat16)
            dv = jnp.dot(p.astype(jnp.bfloat16), do, preferred_element_type=jnp.float32)
            dk = jnp.dot(ds, q, preferred_element_type=jnp.float32)
            if step == 0:
                if not fresh:
                    dk, dv = old_ref[j, 0] + dk, old_ref[j, 1] + dv
                acc[j, 0], acc[j, 1] = dk, dv
            else:
                acc[j, 0] += dk
                acc[j, 1] += dv
            dqt = dqt + jnp.dot(kt[j], ds, preferred_element_type=jnp.float32)
        n, t = piece
        dq = (dqt * scale).T.astype(jnp.bfloat16)
        dq_refs[n][0, t : t + tokens] = dq.reshape(tokens, group, width)
    if last:
        for j, out in enumerate(sum_refs):
            out[0] = (acc[j, 0] * scale).astype(out.dtype)
            out[1] = acc[j, 1].astype(out.dtype)
    else:
        sum_refs[0][...] = acc[...]


def group_grads(pairs, where, distances, window, sums, last):
    count = len(pairs)
    _, _, part_rows, group, width = pairs[0].shape
    tok_rows = window[2].shape[1]
    rows = part_rows * group
    cells = count * rows * 3 * tok_rows
    shape = (2, tok_rows, width)
    if last:
        kinds = [pltpu.VMEM(shape, jnp.bfloat16)] * 2 + [pltpu.VMEM(shape, jnp.float32)]
    else:
        kinds = [pltpu.VMEM((3, *shape), jnp.float32)]
    old = [] if sums is None else [sums]
    outs = pl.pallas_call(
        functools.partial(grads_kernel, where, distances, sums is None, last),
        in_specs=[VMEM] * (count + 3 + len(old)),
        out_specs=[VMEM] * (count + len(kinds)),
        out_shape=[pltpu.VMEM((1, part_rows, group, width), jnp.bfloat16)] * count + kinds,
        scratch_shapes=[
            pltpu.VMEM((3, *shape), jnp.float32),
            pltpu.VMEM((3, width, tok_rows), jnp.bfloat16),
        ],
        compiler_params=pltpu.CompilerParams(vmem_limit_bytes=32 * 2**20),
        cost_estimate=pl.CostEstimate(
            flops=10 * cells * width, bytes_accessed=6 * count * rows * width, transcendentals=cells
        ),
        name="grads",
    )(*pairs, *window, *old)
    return outs[:count], outs[count:]


def shards(queries, key_vector_rows, value_vector_rows, grad_out):
    part_rows, heads, width = queries.shape
    kv_heads = key_vector_rows.shape[1]
    peers = lax.axis_size("head")
    group = heads // (peers * kv_heads)
    places = peers * kv_heads
    queries = queries.reshape(part_rows, places, group, width)
    grad_out = grad_out.reshape(part_rows, places, group, width)
    far_cores = list(range(2, peers))
    all_kv = list(range(kv_heads))

    own, first = pack_first(
        key_vector_rows, value_vector_rows, queries, grad_out, [[(0, d)] for d in far_cores]
    )
    rest = pack(
        queries,
        grad_out,
        [[(kv, 0) for kv in all_kv], [(kv, 1) for kv in all_kv]]
        + [[(kv, d)] for kv in all_kv[1:] for d in far_cores],
        kv_heads,
    )
    sent = [first] + [rest[2 + n * len(far_cores) :][: len(far_cores)] for n in range(kv_heads - 1)]
    crossed, windows = [], []
    for kv in all_kv:
        values = []
        for value, d in zip(sent[kv], far_cores):
            values.append(swapped(value, d))
        crossed.append(values)
        far = shifted(own[kv], 2)
        near = shifted(own[kv], 1)
        windows.append((far, near, own[kv]))
    here = rest[0]
    partner = swapped(rest[1], 1)
    dq, totals = {}, []
    for kv in all_kv:
        final = kv == all_kv[-1]
        turns = [[0, 1]] + [[d] for d in far_cores]
        sums = None
        for turn in turns:
            values = {0: here, 1: partner, **dict(zip(far_cores, crossed[kv]))}
            made, sums = group_grads(
                [values[d] for d in turn],
                [kv if d < 2 else 0 for d in turn],
                turn,
                windows[kv],
                None if sums is None else sums[0],
                turn is turns[-1],
            )
            for d, value in zip(turn, made):
                if d >= 2:
                    value = swapped(value, d)
                dq[kv, d] = value
        dfar = shifted(sums[0], -2)
        dnear = shifted(sums[1], -1)
        totals.append((sums[2], dfar, dnear))
    dq_partner = swapped(jnp.concatenate([dq[kv, 1] for kv in all_kv], axis=0), 1)
    early = [[(kv, 0)] for kv in all_kv] + [[(kv, 1) for kv in all_kv]]
    early += [[(kv, d)] for kv in all_kv[:-1] for d in far_cores]
    values = [dq[part[0]] if len(part) == 1 else dq_partner for part in early]
    stored = store(values, early, places, kv_heads)
    late = [(all_kv[-1], d) for d in far_cores]
    return finish(stored, [dq[key] for key in late], [[key] for key in late], totals)


def solution(mesh):
    return jax.shard_map(
        shards,
        mesh=mesh,
        in_specs=(
            P(("inner", "outer", "head"), None, None),
            P(("inner", "outer"), "head", None),
            P(("inner", "outer"), "head", None),
            P(("inner", "outer", "head"), None, None),
        ),
        out_specs=(
            P(("inner", "outer", "head"), None, None),
            P(("inner", "outer"), "head", None),
            P(("inner", "outer"), "head", None),
        ),
        check_vma=False,
    )
```
